256 devices in a mesh: batch: 8 (over x, y_lo), seq: 16 (over y_hi, z), head: 2 (over core).
Axes of the slice: x: 4, y: 4 (y_hi: 2, y_lo: 2; y = y_hi * 2 + y_lo), z: 8, core: 2. Of those that a mesh axis runs over, the one named last changes fastest.
Arguments:
- queries: bfloat16 [1, 49152, 2048], P(None, ('batch', 'seq'), 'head'), parts along dimension 1, may hold values from -240 to 240
- keys: bfloat16 [1, 49152, 1024], P(None, ('batch', 'seq'), 'head'), parts along dimension 1, may hold values from -6 to 6
- values: bfloat16 [1, 49152, 1024], P(None, ('batch', 'seq'), 'head'), parts along dimension 1, may hold values from -6 to 6
- exit_layer: int32 [384], P(('batch', 'seq')), parts along dimension 0, may hold values from 0 to 1
- tile_order: int32 [384], P('batch'), parts along dimension 0, may hold values from 0 to 47, each once
Outputs:
- attended: bfloat16 [1, 49152, 2048], P(None, ('batch', 'seq'), 'head'), parts along dimension 1
- live_tiles: int32 [8], P('batch'), parts along dimension 0
The draws below stay inside these ranges and needn't reach their ends.
There are 8 independent parts, one for each index of `batch`. The reference program is written for one: setup_inputs(seed, part) draws one part's arguments, and reference() takes and returns one part's arrays. A program takes and returns all parts, laid end to end along the dimension named above; each array names one. Nothing has to cross between parts.
Inputs may be any that keep to these rules, and one draw needn't show every extreme that they name: Tile t covers tokens t * 128 to t * 128 + 127 of the token dimension; tile_order is a permutation of 0 to 47.
All inputs are finite; a program needn't handle non-finite values.
Results may differ from the reference program's by a relative error of at most 0.0049.
Values may be sent and summed in bfloat16 or wider, within the bound.
A program may use at most 128 MiB of HBM per device.

```python
import math
import jax
import jax.numpy as jnp
from jax import lax

LAYERS = 1
QH = 8
KVH = 4
HD = 256
TILE = 128
TOKENS = 6144
TILES = 48
KW = 1024


def draw_queries(key, part):
    query_key = jax.random.fold_in(key, 101)
    base = jnp.clip(jax.random.normal(query_key, (LAYERS, TOKENS, QH * HD), jnp.float32), -6.0, 6.0)
    return base.astype(jnp.bfloat16)


def draw_exit_layer(key, part):
    exit_key = jax.random.fold_in(key, 202)
    tile_ids = jnp.arange(TILES, dtype=jnp.int32)
    lowest = tile_ids * LAYERS // TILES
    spread = LAYERS + 1 - lowest
    raw_bits = jax.random.randint(exit_key, (TILES,), 0, 1 << 20, dtype=jnp.int32)
    return (lowest + raw_bits % spread).astype(jnp.int32)


def levels(own_key, shape, pieces, low, largest):
    def one(dim, parts):
        draws = jax.random.uniform(jax.random.fold_in(jax.random.fold_in(own_key, 6), dim), (parts,), jnp.float32, low / len(pieces), largest / len(pieces))
        return jnp.repeat(jnp.exp(draws), shape[dim] // parts).reshape((-1,) + (1,) * (len(shape) - dim - 1))

    gain = one(*pieces[0])
    for cut in pieces[1:]:
        gain = gain * one(*cut)
    return gain


def bell_draw(own_key, shape, width, reach, shards=(), held_as=jnp.bfloat16):
    drawn = width * jax.random.normal(own_key, shape, jnp.float32)
    if shards:
        drawn = drawn * levels(own_key, shape, shards, -0.22, 0.18)
    return jnp.clip(drawn, -reach, reach).astype(held_as)


def setup_inputs(seed: int = 0, part: int = 0) -> dict:
    streams_of = jax.random.split(jax.random.key(seed), 6)
    part_keys = jax.random.split(jax.random.fold_in(streams_of[5], part), 6)
    queries = draw_queries(jax.random.fold_in(jax.random.fold_in(streams_of[5], part), 71), part)
    keys = bell_draw(part_keys[1], (LAYERS, TOKENS, KW), 1.0, 6.0, ((1, 16), (2, 2)))
    values = bell_draw(part_keys[2], (LAYERS, TOKENS, KW), 1.0, 6.0, ((1, 16), (2, 2)))
    exit_layer = draw_exit_layer(jax.random.fold_in(jax.random.fold_in(streams_of[5], part), 71), part)
    tile_order = jax.random.permutation(part_keys[4], TILES).astype(jnp.int32)
    return dict(queries=queries, keys=keys, values=values, exit_layer=exit_layer, tile_order=tile_order)


softcap = 50.0
query_scale = 0.0625


def reference(queries, keys, values, exit_layer, tile_order):
    group_size = QH // KVH
    offsets = jnp.arange(TOKENS, dtype=jnp.int32)
    positions = (tile_order[offsets // TILE] * TILE + offsets % TILE).astype(jnp.int32)
    token_exits = exit_layer[offsets // TILE]
    block_rows = math.gcd(TOKENS, 512)
    outputs = []
    for layer_id in range(LAYERS):
        key_heads = keys[layer_id].reshape(TOKENS, KVH, HD).astype(jnp.float32)
        value_heads = values[layer_id].reshape(TOKENS, KVH, HD).astype(jnp.float32)
        query_blocks = queries[layer_id].reshape(TOKENS // block_rows, block_rows, KVH, group_size, HD)
        query_pos = positions.reshape(TOKENS // block_rows, block_rows)

        def one_block(operands):
            query_block, pos_block = operands
            scores = jnp.einsum("tkgd,skd->kgts", query_block.astype(jnp.float32), key_heads) * query_scale
            allowed = positions[None, :] <= pos_block[:, None]
            weights = jnp.where(allowed[None, None], jnp.exp(softcap * jnp.tanh(scores / softcap)), 0.0)
            denominator = jnp.sum(weights, axis=-1)
            rounded = lax.optimization_barrier(weights.astype(jnp.bfloat16))
            numerator = jnp.einsum("kgts,skd->kgtd", rounded.astype(jnp.float32), value_heads)
            output = numerator / denominator[..., None]
            return jnp.transpose(output, (2, 0, 1, 3)).reshape(block_rows, QH * HD)

        attended_layer = lax.map(one_block, (query_blocks, query_pos)).reshape(TOKENS, QH * HD)
        attended_layer = jnp.where((token_exits > layer_id)[:, None], attended_layer, 0.0)
        outputs.append(attended_layer.astype(jnp.bfloat16))
    live_tiles = jnp.stack([jnp.sum((exit_layer > layer_id).astype(jnp.int32)) for layer_id in range(LAYERS)])
    return jnp.stack(outputs), live_tiles.astype(jnp.int32)
```

```python
import math

import jax
import jax.numpy as jnp
from jax import lax
from jax.experimental import pallas as pl
from jax.experimental.pallas import tpu as pltpu
from jax.sharding import PartitionSpec as P

MESH = pl.DeviceIdType.MESH
HD = 256
TILE = 128
ROWS = 384
OWN_TILES = 3
Z = 8
SEQ = 16
PAIRS = 12
OWN_SLOT = (1, 22, 0)
SCORE_TO_TANH = 0.0625 / 50.0
TANH_TO_EXP2 = 50.0 * math.log2(math.e)


def kernel(
    q_hbm, k_hbm, v_hbm, exit_ref, order_ref,
    out_ref, live_ref,
    q, kv, acc, den, q_relay, o_send, o_relay, o_back, d_send, d_relay, d_back, counts,
    ld_q, ld_kv, z_out, z_in, q_out, q_in, o_out, o_in, c_out, c_in,
):
    batch = lax.axis_index("batch")
    seq = lax.axis_index("seq")
    y_lo = lax.rem(batch, 2)
    y_hi = seq // Z
    z = lax.rem(seq, Z)
    other_batch = batch + 1 - 2 * y_lo
    up = {"seq": y_hi * Z + lax.rem(z + 1, Z)}
    down = {"seq": y_hi * Z + lax.rem(z + Z - 1, Z)}
    y_up = {"batch": other_batch, "seq": lax.rem(y_hi + y_lo, 2) * Z + z}
    y_down = {"batch": other_batch, "seq": lax.rem(y_hi + 1 - y_lo, 2) * Z + z}
    z_to = (up, down)
    y_to = (y_up, y_down)

    def rows(t):
        return pl.ds(t * TILE, TILE)

    loads_kv = {}
    for h in range(2):
        for t in range(OWN_TILES):
            for which, src in ((0, k_hbm), (1, v_hbm)):
                loads_kv[h, t, which] = pltpu.make_async_copy(
                    src.at[rows(t), pl.ds(h * HD, HD)],
                    kv.at[h, which, OWN_SLOT[t]],
                    ld_kv.at[h, t, which],
                )
    loads_q = [
        pltpu.make_async_copy(q_hbm.at[:, pl.ds(n * HD, HD)], q.at[0, n], ld_q.at[n])
        for n in range(4)
    ]
    for t in range(OWN_TILES):
        for which in range(2):
            loads_kv[0, t, which].start()
    for n in range(4):
        loads_q[n].start()
    for t in range(OWN_TILES):
        for which in range(2):
            loads_kv[1, t, which].start()

    barrier = pltpu.get_barrier_semaphore()

    def greet(n, c):
        pl.semaphore_signal(
            barrier, inc=1, device_id={"seq": lax.rem(seq + n, SEQ)}, device_id_type=MESH
        )
        return c

    for peer in y_to:
        pl.semaphore_signal(barrier, inc=1, device_id=peer, device_id_type=MESH)
    lax.fori_loop(1, SEQ, greet, 0)

    local_live = jnp.int32(0)
    for t in range(OWN_TILES):
        local_live = local_live + (exit_ref[t] > 0).astype(jnp.int32)
    counts[seq] = jnp.full((8, 128), local_live, jnp.int32)

    pl.semaphore_wait(barrier, SEQ + 1)

    def z_copy(way, h, src_slot, i):
        dst_slot = 2 * (i + 1) + (i // 10 if way == 0 else 1)
        return pltpu.make_async_remote_copy(
            src_ref=kv.at[h, :, src_slot],
            dst_ref=kv.at[h, :, dst_slot],
            send_sem=z_out.at[way, h, i],
            recv_sem=z_in.at[way, h, i],
            device_id=z_to[way],
            device_id_type=MESH,
        )

    def z_slot(way, i):
        return 2 * (i + 1) + (i // 10 if way == 0 else 1)

    def q_first(way, g, t):
        return pltpu.make_async_remote_copy(
            src_ref=q.at[0, 2 * g + way, rows(t)],
            dst_ref=q_relay.at[way, g, t],
            send_sem=q_out.at[0, way, g, t],
            recv_sem=q_in.at[0, way, g, t],
            device_id=y_to[way],
            device_id_type=MESH,
        )

    def q_second(way, g, t):
        return pltpu.make_async_remote_copy(
            src_ref=q_relay.at[way, g, t],
            dst_ref=q.at[1, 2 * g + way, rows(t)],
            send_sem=q_out.at[1, way, g, t],
            recv_sem=q_in.at[1, way, g, t],
            device_id=y_to[way],
            device_id_type=MESH,
        )

    def o_first(way, g, t):
        n = 2 * g + way
        src, dst = (
            (o_send.at[n, rows(t)], o_relay.at[way, g, t])
            if t < OWN_TILES
            else (d_send.at[n], d_relay.at[n])
        )
        return pltpu.make_async_remote_copy(
            src_ref=src,
            dst_ref=dst,
            send_sem=o_out.at[0, way, g, t],
            recv_sem=o_in.at[0, way, g, t],
            device_id=y_to[way],
            device_id_type=MESH,
        )

    def o_second(way, g, t):
        n = 2 * g + way
        src, dst = (
            (o_relay.at[way, g, t], o_back.at[n, rows(t)])
            if t < OWN_TILES
            else (d_relay.at[n], d_back.at[n])
        )
        return pltpu.make_async_remote_copy(
            src_ref=src,
            dst_ref=dst,
            send_sem=o_out.at[1, way, g, t],
            recv_sem=o_in.at[1, way, g, t],
            device_id=y_to[way],
            device_id_type=MESH,
        )

    def send_own(h, j):
        for way in range(2):
            z_copy(way, h, OWN_SLOT[j if way == 0 else 2 - j], j).start()

    for t in (0, 2, 1):
        for which in range(2):
            loads_kv[0, t, which].wait()
    for j in range(OWN_TILES):
        send_own(0, j)
    for n in range(4):
        loads_q[n].wait()
    for t in range(OWN_TILES):
        for way in range(2):
            q_first(way, 0, t).start()

    def count_copy(n):
        return pltpu.make_async_remote_copy(
            src_ref=counts.at[seq],
            dst_ref=counts.at[seq],
            send_sem=c_out.at[n],
            recv_sem=c_in.at[n],
            device_id={"seq": lax.rem(seq + n, SEQ)},
            device_id_type=MESH,
        )

    def send_count(n, c):
        count_copy(n).start()
        return c

    lax.fori_loop(1, SEQ, send_count, 0)

    for t in range(OWN_TILES):
        for which in range(2):
            loads_kv[1, t, which].wait()

    acc[...] = jnp.zeros_like(acc)
    den[...] = jnp.zeros_like(den)

    ahead = lax.broadcasted_iota(jnp.int32, (TILE, TILE), 1) - lax.broadcasted_iota(
        jnp.int32, (TILE, TILE), 0
    )

    def work(src, h, p):
        column = lax.rem(y_hi + src, 2)
        away = (p + 2) // 3
        t0 = lax.rem(p + 2, 3)
        away_low = jnp.where(p == PAIRS - 1, 0, away)
        k_tiles = (
            (y_hi * Z + lax.rem(z + Z - away_low, Z)) * OWN_TILES + t0,
            (y_hi * Z + lax.rem(z + away, Z)) * OWN_TILES + 2 - t0,
        )
        query = q[src, pl.ds(2 * h, 2)].reshape(2 * ROWS, HD)
        key = kv[h, 0, pl.ds(2 * p, 2)].reshape(2 * TILE, HD)
        value = kv[h, 1, pl.ds(2 * p, 2)].reshape(2 * TILE, HD)
        score = lax.dot_general(
            query, key, (((1,), (1,)), ((), ())), preferred_element_type=jnp.float32
        )
        weight = jnp.exp2(jnp.tanh(score * SCORE_TO_TANH) * TANH_TO_EXP2)
        k_order = [order_ref[n] for n in k_tiles]
        masks = []
        for t in range(OWN_TILES):
            q_order = order_ref[(column * Z + z) * OWN_TILES + t]
            masks.append([ahead <= (q_order - k) * TILE for k in k_order])
        blocks = []
        for head in range(2):
            for t in range(OWN_TILES):
                lower = (head * OWN_TILES + t) * TILE
                both = weight[lower : lower + TILE]
                left = jnp.where(masks[t][0], both[:, :TILE], 0.0)
                right = jnp.where(masks[t][1], both[:, TILE:], 0.0)
                den[src, 2 * h + head, rows(t)] += left + right
                blocks.append(jnp.concatenate([left, right], axis=1).astype(jnp.bfloat16))
        product = jnp.dot(
            jnp.concatenate(blocks, axis=0), value, preferred_element_type=jnp.float32
        )
        acc[src, pl.ds(2 * h, 2)] += product.reshape(2, ROWS, HD)

    def give_back(g):
        for way in range(2):
            n = 2 * g + way
            for t in range(OWN_TILES):
                o_send[n, rows(t)] = acc[1, n, rows(t)].astype(jnp.bfloat16)
                o_first(way, g, t).start()
        for way in range(2):
            n = 2 * g + way
            for t in range(OWN_TILES):
                total = jnp.sum(jnp.transpose(den[1, n, rows(t)]), axis=0, keepdims=True)
                d_send[n, :, rows(t)] = jnp.broadcast_to(total, (8, TILE))
            o_first(way, g, OWN_TILES).start()

    def step(u, c):
        h = u // PAIRS
        p = lax.rem(u, PAIRS)
        i = p - 1

        @pl.when((p >= 1) & (p <= PAIRS - 2))
        def _():
            for way in range(2):
                z_copy(way, h, 0, i).wait_recv()

                @pl.when(i + 3 <= (10 - h if way == 0 else 9 + h))
                def _():
                    z_copy(way, h, z_slot(way, i), i + 3).start()

        for way in range(2):

            @pl.when((p == PAIRS - 1) & (h == way))
            def _():
                z_copy(way, way, 0, 10).wait_recv()

        for j in range(OWN_TILES):

            @pl.when(u == 6 + j)
            def _():
                send_own(1, j)

        @pl.when(u == 1)
        def _():
            for t in range(OWN_TILES):
                for way in range(2):
                    q_first(way, 0, t).wait_recv()
                    q_second(way, 0, t).start()
            for t in range(OWN_TILES):
                for way in range(2):
                    q_first(way, 1, t).start()

        @pl.when(u == 3)
        def _():
            for t in range(OWN_TILES):
                for way in range(2):
                    q_first(way, 1, t).wait_recv()
                    q_second(way, 1, t).start()

        for g, at in ((0, 5), (1, PAIRS)):

            @pl.when(u == at)
            def _():
                for t in range(OWN_TILES):
                    for way in range(2):
                        q_second(way, g, t).wait_recv()

        @pl.when(u == PAIRS + 3)
        def _():
            for t in range(OWN_TILES + 1):
                for way in range(2):
                    o_first(way, 0, t).wait_recv()
                    o_second(way, 0, t).start()

        @pl.when(u < 2 * PAIRS - 1)
        def _():
            work(0, h, p)

        first = jnp.where(u < 5, 0, jnp.where(u < 10, 2 * (u - 5), u))
        many = jnp.where(u < 5, 0, jnp.where(u < 10, 2, 1))

        def remote(n, c):
            work(1, (first + n) // PAIRS, lax.rem(first + n, PAIRS))
            return c

        lax.fori_loop(0, many, remote, 0)

        @pl.when(u == PAIRS - 1)
        def _():
            give_back(0)

        return c

    lax.fori_loop(0, 2 * PAIRS, step, 0)
    give_back(1)
    work(0, 1, PAIRS - 1)

    def wait_count(n, c):
        count_copy(n).wait_recv()
        return c

    lax.fori_loop(1, SEQ, wait_count, 0)
    total = counts[0]
    for n in range(1, SEQ):
        total = total + counts[n]
    live_ref[...] = total

    def finish(g):
        for way in range(2):
            n = 2 * g + way
            o_second(way, g, OWN_TILES).wait_recv()
            for t in range(OWN_TILES):
                o_second(way, g, t).wait_recv()
                mine = jnp.sum(den[0, n, rows(t)], axis=1, keepdims=True)
                theirs = jnp.transpose(
                    jnp.broadcast_to(d_back[n, 0:1, rows(t)], (TILE, TILE))
                )
                inverse = 1.0 / (theirs + mine)
                alive = jnp.full((TILE, TILE), exit_ref[t], jnp.int32) > 0
                for half in range(2):
                    lanes = pl.ds(half * TILE, TILE)
                    top = acc[0, n, rows(t), lanes] + o_back[n, rows(t), lanes].astype(
                        jnp.float32
                    )
                    out_ref[rows(t), pl.ds(n * HD + half * TILE, TILE)] = jnp.where(
                        alive, top * inverse, 0.0
                    ).astype(jnp.bfloat16)

    finish(0)
    for t in range(OWN_TILES + 1):
        for way in range(2):
            o_first(way, 1, t).wait_recv()
            o_second(way, 1, t).start()
    finish(1)

    for way in range(2):
        for h in range(2):

            def z_sent(i, c):
                z_copy(way, h, 0, i).wait_send()
                return c

            lax.fori_loop(0, 11 if way == h else 10, z_sent, 0)
        for g in range(2):
            for t in range(OWN_TILES):
                q_first(way, g, t).wait_send()
                q_second(way, g, t).wait_send()
            for t in range(OWN_TILES + 1):
                o_first(way, g, t).wait_send()
                o_second(way, g, t).wait_send()

    def count_sent(n, c):
        count_copy(n).wait_send()
        return c

    lax.fori_loop(1, SEQ, count_sent, 0)


def body(queries, keys, values, exit_layer, tile_order):
    hbm = pl.BlockSpec(memory_space=pltpu.HBM)
    smem = pl.BlockSpec(memory_space=pltpu.SMEM)
    vmem = pl.BlockSpec(memory_space=pltpu.VMEM)
    bf16, f32 = jnp.bfloat16, jnp.float32
    dma = pltpu.SemaphoreType.DMA
    attended, live = pl.pallas_call(
        kernel,
        out_shape=(
            jax.ShapeDtypeStruct((ROWS, 4 * HD), bf16),
            jax.ShapeDtypeStruct((8, 128), jnp.int32),
        ),
        in_specs=[hbm, hbm, hbm, smem, smem],
        out_specs=(vmem, vmem),
        scratch_shapes=[
            pltpu.VMEM((2, 4, ROWS, HD), bf16),
            pltpu.VMEM((2, 2, 2 * PAIRS, TILE, HD), bf16),
            pltpu.VMEM((2, 4, ROWS, HD), f32),
            pltpu.VMEM((2, 4, ROWS, TILE), f32),
            pltpu.VMEM((2, 2, OWN_TILES, TILE, HD), bf16),
            pltpu.VMEM((4, ROWS, HD), bf16),
            pltpu.VMEM((2, 2, OWN_TILES, TILE, HD), bf16),
            pltpu.VMEM((4, ROWS, HD), bf16),
            pltpu.VMEM((4, 8, ROWS), f32),
            pltpu.VMEM((4, 8, ROWS), f32),
            pltpu.VMEM((4, 8, ROWS), f32),
            pltpu.VMEM((SEQ, 8, 128), jnp.int32),
            dma((4,)),
            dma((2, OWN_TILES, 2)),
            dma((2, 2, 11)),
            dma((2, 2, 11)),
            dma((2, 2, 2, OWN_TILES)),
            dma((2, 2, 2, OWN_TILES)),
            dma((2, 2, 2, OWN_TILES + 1)),
            dma((2, 2, 2, OWN_TILES + 1)),
            dma((SEQ,)),
            dma((SEQ,)),
        ],
        compiler_params=pltpu.CompilerParams(collective_id=0, has_side_effects=True),
        cost_estimate=pl.CostEstimate(
            flops=9_663_676_416, bytes_accessed=3_145_728, transcendentals=18_874_368
        ),
        name="attend",
    )(queries[0], keys[0], values[0], exit_layer, tile_order)
    return attended[None], live[0, :1]


def solution(mesh):
    parts = ("batch", "seq")
    return jax.shard_map(
        body,
        mesh=mesh,
        in_specs=(
            P(None, parts, "head"),
            P(None, parts, "head"),
            P(None, parts, "head"),
            P(parts),
            P("batch"),
        ),
        out_specs=(P(None, parts, "head"), P("batch")),
        check_vma=False,
    )
```

```python
import math

import jax
import jax.numpy as jnp
from jax import lax
from jax.experimental import pallas as pl
from jax.experimental.pallas import tpu as pltpu
from jax.sharding import PartitionSpec as P

MESH = pl.DeviceIdType.MESH
HD = 256
TILE = 128
ROWS = 384
TILES = 3
Z = 8
PAIRS = 12
SLOTS = 2 * PAIRS
SCORE_TO_TANH = 0.0625 / 50.0
TANH_TO_EXP2 = 50.0 * math.log2(math.e)

OWN_SLOT = (0, 1, 17)
FOUR_SLOT = (14, 16, 15)
FIRST_PAIR = {1: 1, 2: 4, 3: 9}
HELD_LAG = 2
END_LAG = 4
SEND_FIRST = (1, 2, 3)
SEND_AT = {1: (4,), 2: (5, 7), 3: (6, 8), 5: (9,), 6: (10,), 7: (11,)}


def slot_of(away, t, side):
    return 2 * (FIRST_PAIR[away] + t) + side


def slot_sources():
    found = {}
    for t in range(TILES):
        found[OWN_SLOT[t]] = (0, t)
        found[FOUR_SLOT[t]] = (4, t)
        for away in (1, 2, 3):
            found[slot_of(away, t, 0)] = (Z - away, t)
            found[slot_of(away, t, 1)] = (away, t)
    return found


def rows(t):
    return pl.ds(t * TILE, TILE)


def kernel(
    q_hbm, k_hbm, v_hbm, exit_ref, order_ref,
    out_hbm, live_ref,
    q_mine, kv_mine, q, kv, acc, den, y_held, four_held, o_send, exits, column, k_order, q_order,
    mine_in, q_mine_in, own_in, own_q_in, own_y_out, z_out, z_in, four_out, four_in, four_on, f_out, f_in,
    y_out, y_in, y_on, y_end, q_out, q_in, o_out, o_in, o_local, e_out, e_in, c_out, c_in,
):
    batch = lax.axis_index("batch")
    seq = lax.axis_index("seq")
    core = lax.axis_index("head")
    y_lo = lax.rem(batch, 2)
    y_hi = seq // Z
    z = lax.rem(seq, Z)
    hosted = lax.rem(z, 4)
    home = core == hosted // 2
    sibling = {"head": 1 - core}
    other_batch = batch + 1 - 2 * y_lo
    y_to = (
        {"batch": other_batch, "seq": lax.rem(y_hi + y_lo, 2) * Z + z},
        {"batch": other_batch, "seq": lax.rem(y_hi + 1 - y_lo, 2) * Z + z},
    )

    def chip(offset):
        return y_hi * Z + lax.rem(z + offset, Z)

    def remote(src, dst, sent, arrived, device):
        return pltpu.make_async_remote_copy(
            src_ref=src, dst_ref=dst, send_sem=sent, recv_sem=arrived,
            device_id=device, device_id_type=MESH,
        )

    def columns(n):
        return pl.ds(pl.multiple_of(n * HD, HD), HD)

    q_from = (0, Z - 1, 1, Z - 2 - 4 * core)

    own_column = lax.rem(hosted, 2)
    own_loads = [
        pltpu.make_async_copy(
            src.at[rows(t), columns(own_column)], kv.at[part, OWN_SLOT[t]], own_in.at[t, part]
        )
        for t in range(TILES)
        for part, src in ((0, k_hbm), (1, v_hbm))
    ]
    own_q_load = pltpu.make_async_copy(
        q_hbm.at[:, columns(2 * own_column + core)], q.at[0], own_q_in.at[0]
    )

    loads = [
        pltpu.make_async_copy(
            src.at[rows(t), pl.ds(j * HD, HD)], kv_mine.at[part, j, t], mine_in.at[part, j, t]
        )
        for t in range(TILES)
        for j in range(2)
        for part, src in ((0, k_hbm), (1, v_hbm))
    ] + [
        pltpu.make_async_copy(q_hbm.at[:, pl.ds(n * HD, HD)], q_mine.at[n], q_mine_in.at[n])
        for n in range(4)
    ]
    for load in loads:
        load.start()

    @pl.when(home)
    def _():
        for load in own_loads:
            load.start()
        own_q_load.start()

    sublane = lax.broadcasted_iota(jnp.int32, (8, 128), 0)
    mine = jnp.zeros((8, 128), jnp.int32)
    for t in range(TILES):
        mine = jnp.where(sublane == t, exit_ref[t], mine)
    exits[0] = mine

    barrier = pltpu.get_barrier_semaphore()
    near = (1, 2, 3, 5, 6, 7)
    for offset in near:
        for c in range(2):
            pl.semaphore_signal(
                barrier, inc=1, device_id={"seq": chip(offset), "head": c}, device_id_type=MESH
            )
    for peer in y_to:
        for c in range(2):
            pl.semaphore_signal(
                barrier, inc=1, device_id={**peer, "head": c}, device_id_type=MESH
            )
    pl.semaphore_signal(barrier, inc=1, device_id=sibling, device_id_type=MESH)
    for load in loads:
        load.wait()
    pl.semaphore_wait(barrier, 2 * len(near) + 5)

    def q_copy(n, offset, c, index):
        head = lax.rem(z + offset, 4)
        return remote(
            q_mine.at[2 * lax.rem(head, 2) + c],
            q.at[index],
            q_out.at[n],
            q_in.at[index],
            {"seq": chip(offset), "head": c},
        )

    q_sends = []
    for n, (offset, c, index) in enumerate(
        ((2, 0, 3), (6, 1, 3), (1, 0, 1), (1, 1, 1), (7, 0, 2), (7, 1, 2))
    ):
        q_sends.append((lax.rem(z + offset, 4) // 2 == core, q_copy(n, offset, c, index)))
    own_q_send = remote(
        q_mine.at[2 * own_column + 1 - core], q.at[0], q_out.at[6], q_in.at[0], sibling
    )
    own_y_sends = [
        remote(
            kv_mine.at[part, own_column, t], y_held.at[OWN_SLOT[t]],
            own_y_out.at[t, part], y_in.at[OWN_SLOT[t]],
            {**y_to[OWN_SLOT[t] % 2], "head": part},
        )
        for t in range(TILES)
        for part in range(2)
    ]

    @pl.when(home)
    def _():
        for copy in own_y_sends:
            copy.start()

    for holds, copy in q_sends:

        @pl.when(holds)
        def _():
            copy.start()

    pl.when(home)(own_q_send.start)

    def z_copies(away):
        found = []
        for t in range(TILES):
            for side in range(2):
                offset = away if side == 0 else Z - away
                head = lax.rem(z + offset, 4)
                for part in range(2):
                    slot = slot_of(away, t, side)
                    found.append((
                        head // 2 == core,
                        remote(
                            kv_mine.at[part, lax.rem(head, 2), t],
                            kv.at[part, slot],
                            z_out.at[part, slot],
                            z_in.at[slot],
                            {"seq": chip(offset), "head": part},
                        ),
                    ))
        return found

    def four_copies():
        found = []
        for n in range(2):
            for way in range(2):
                offset = 2 if way == 0 else Z - 2
                for part in range(2):
                    if n == 1 and part != way:
                        continue
                    t = 1 if n == 1 else 2 * way
                    found.append((
                        home,
                        remote(
                            kv_mine.at[part, own_column, t],
                            four_held.at[way, n],
                            four_out.at[way, n, part],
                            four_in.at[way, n],
                            {"seq": chip(offset), "head": part},
                        ),
                    ))
        return found

    by_pair = {}
    for away in (1, 2, 3):
        copies = z_copies(away)
        for t in range(TILES):
            by_pair[FIRST_PAIR[away] + t] = copies[4 * t : 4 * t + 4]
    four = four_copies()
    by_pair[7], by_pair[8] = four[:4], four[4:]
    kv_sends = [copy for copies in by_pair.values() for copy in copies]

    def start_all(copies):
        for holds, copy in copies:
            pl.when(holds)(copy.start)

    def f_copy(slot):
        return remote(
            kv.at[core, slot], kv.at[core, slot], f_out.at[slot], f_in.at[slot], sibling
        )

    def f_arrived(slot):
        return remote(
            kv.at[1 - core, slot], kv.at[1 - core, slot], f_out.at[slot], f_in.at[slot], sibling
        )

    def own_copy(t):
        slot = OWN_SLOT[t]
        return remote(
            kv.at[1 - core, slot], kv.at[1 - core, slot],
            z_out.at[0, slot], z_in.at[slot], sibling,
        )

    def z_arrived(slot):
        return remote(
            kv.at[core, slot], kv.at[core, slot], f_out.at[slot], z_in.at[slot], sibling
        )

    def y_first(slot, side):
        return remote(
            kv.at[core, slot], y_held.at[slot], y_out.at[slot], y_in.at[slot], y_to[side]
        )

    def y_second(slot, side):
        return remote(
            y_held.at[slot], kv.at[core, SLOTS + slot], y_on.at[slot], y_end.at[slot], y_to[side]
        )

    def four_forward(way, n):
        slot = FOUR_SLOT[1] if n == 1 else FOUR_SLOT[2 * way]
        return remote(
            four_held.at[way, n], kv.at[core, slot], four_on.at[way, n], z_in.at[slot],
            {"seq": chip(2 if way == 0 else Z - 2)},
        )

    for pair in SEND_FIRST:
        start_all(by_pair[pair])

    def exit_copy(offset):
        back = Z - offset
        return remote(
            exits.at[0], exits.at[back], e_out.at[offset], e_in.at[back], {"seq": chip(offset)}
        )

    exit_on = remote(exits.at[2], exits.at[4], e_out.at[4], e_in.at[4], {"seq": chip(Z - 2)})
    for offset in near:
        exit_copy(offset).start()

    @pl.when(home)
    def _():
        for load in own_loads:
            load.wait()
        for t in range(TILES):
            own_copy(t).start()
            f_copy(OWN_SLOT[t]).start()

    @pl.when(jnp.logical_not(home))
    def _():
        for t in range(TILES):
            z_arrived(OWN_SLOT[t]).wait_recv()

    acc[...] = jnp.zeros_like(acc)
    den[...] = jnp.zeros_like(den)
    for slot, (offset, t) in slot_sources().items():
        there = lax.rem(z + offset, Z)
        for other in range(2):
            k_order[other * SLOTS + slot] = order_ref[
                (lax.rem(y_hi + other, 2) * Z + there) * TILES + t
            ]
    for m, offset in enumerate(q_from):
        for t in range(TILES):
            q_order[m * TILES + t] = order_ref[chip(offset) * TILES + t]

    ahead = lax.broadcasted_iota(jnp.int32, (TILE, TILE), 1) - lax.broadcasted_iota(
        jnp.int32, (TILE, TILE), 0
    )

    def work(pair, half):
        query = q[pl.ds(2 * half, 2)].reshape(2 * ROWS, HD)
        key = kv[0, pl.ds(2 * pair, 2)].reshape(2 * TILE, HD)
        value = kv[1, pl.ds(2 * pair, 2)].reshape(2 * TILE, HD)
        score = lax.dot_general(
            query, key, (((1,), (1,)), ((), ())), preferred_element_type=jnp.float32
        )
        weight = jnp.exp2(jnp.tanh(score * SCORE_TO_TANH) * TANH_TO_EXP2)
        left_order = k_order[2 * pair]
        right_order = k_order[2 * pair + 1]
        blocks = []
        for m in range(2):
            for t in range(TILES):
                lower = (m * TILES + t) * TILE
                both = weight[lower : lower + TILE]
                mine = q_order[(2 * half + m) * TILES + t]
                left = jnp.where(ahead <= (mine - left_order) * TILE, both[:, :TILE], 0.0)
                right = jnp.where(ahead <= (mine - right_order) * TILE, both[:, TILE:], 0.0)
                den[2 * half + m, rows(t)] += left + right
                blocks.append(jnp.concatenate([left, right], axis=1).astype(jnp.bfloat16))
        product = jnp.dot(
            jnp.concatenate(blocks, axis=0), value, preferred_element_type=jnp.float32
        )
        acc[pl.ds(2 * half, 2)] += product.reshape(2, ROWS, HD)

    def both_parts(pair):
        for side in range(2):
            slot = 2 * pair + side
            owned = (slot == OWN_SLOT[0]) | (slot == OWN_SLOT[1]) | (slot == OWN_SLOT[2])

            @pl.when(jnp.logical_not(owned & home))
            def _():
                f_arrived(slot).wait_recv()

    def each_slot(p, act):
        for side in range(2):

            @pl.when(jnp.logical_not((p == 8) & (side == 1)))
            def _():
                act(2 * p + side, side)

        @pl.when(p == 0)
        def _():
            act(OWN_SLOT[2], 1)

    def arrive_z(slot, side):
        z_arrived(slot).wait_recv()
        f_copy(slot).start()
        y_first(slot, side).start()

    def arrive_held(slot, side):
        y_first(slot, side).wait_recv()
        y_second(slot, side).start()

    def arrive_y(slot, side):
        y_second(slot, side).wait_recv()
        f_copy(SLOTS + slot).start()

    def step(p, carry):
        @pl.when(p == 7)
        def _():
            for way in range(2):
                four_forward_in = remote(
                    four_held.at[way, 0], four_held.at[way, 0],
                    four_on.at[way, 0], four_in.at[way, 0], sibling,
                )
                four_forward_in.wait_recv()
                four_forward(way, 0).start()
            for way in range(2):

                @pl.when(core == way)
                def _():
                    remote(
                        four_held.at[way, 1], four_held.at[way, 1],
                        four_on.at[way, 1], four_in.at[way, 1], sibling,
                    ).wait_recv()
                    four_forward(way, 1).start()

        @pl.when(p >= END_LAG)
        def _():
            each_slot(p - END_LAG, arrive_y)

        @pl.when((p >= HELD_LAG) & (p < PAIRS + HELD_LAG))
        def _():
            each_slot(p - HELD_LAG, arrive_held)

        @pl.when((p >= 1) & (p <= PAIRS - 1))
        def _():
            each_slot(p, arrive_z)

        for at, pairs in SEND_AT.items():

            @pl.when(p == at)
            def _():
                for pair in pairs:
                    start_all(by_pair[pair])

        @pl.when(p == 1)
        def _():
            pl.when(home)(own_q_load.wait)
            for m in range(4):

                @pl.when(jnp.logical_not(home) if m == 0 else m > 0)
                def _():
                    remote(q.at[m], q.at[m], q_out.at[m], q_in.at[m], sibling).wait_recv()

        @pl.when((p >= 1) & (p <= PAIRS))
        def _():
            both_parts(p - 1)

        @pl.when(p > END_LAG)
        def _():
            both_parts(PAIRS + p - END_LAG - 1)

        first = jnp.where((p >= 1) & (p <= PAIRS), 0, 2)
        last = jnp.where(p > END_LAG, 4, 2)

        def item(n, c):
            work(jnp.where(n < 2, p - 1, PAIRS + p - END_LAG - 1), lax.rem(n, 2))
            return c

        lax.fori_loop(first, last, item, 0)

        @pl.when(p == 3)
        def _():
            remote(exits.at[2], exits.at[2], e_out.at[2], e_in.at[2], sibling).wait_recv()
            exit_on.start()

        @pl.when(p == 6)
        def _():
            for offset in (1, 3, 4, 5, 6, 7):
                remote(
                    exits.at[offset], exits.at[offset],
                    e_out.at[offset], e_in.at[offset], sibling,
                ).wait_recv()
            alive = jnp.zeros((8, 128), jnp.int32)
            for offset in range(Z):
                alive = alive + (exits[offset] > 0).astype(jnp.int32)
            column[0] = jnp.broadcast_to(jnp.sum(alive, axis=0, keepdims=True), (8, 128))

        pl.when(p == 7)(count_first.start)

        @pl.when(p == 9)
        def _():
            count_first.wait_recv()
            count_second.start()

        return carry

    count_first = remote(column.at[0], column.at[1], c_out.at[0], c_in.at[0], y_to[0])
    count_second = remote(column.at[1], column.at[2], c_out.at[1], c_in.at[1], y_to[0])

    lax.fori_loop(0, PAIRS + END_LAG, step, 0)

    def o_copy(m, t):
        return remote(
            o_send.at[m, rows(t)],
            out_hbm.at[rows(t), columns(2 * own_column + core)],
            o_out.at[m, t],
            o_in.at[2 * own_column + core, t],
            {"seq": chip(q_from[m]), "head": hosted // 2},
        )

    def o_here(t):
        return pltpu.make_async_copy(
            o_send.at[0, rows(t)],
            out_hbm.at[rows(t), columns(2 * own_column + core)],
            o_local.at[t],
        )

    def finish(m):
        for t in range(TILES):
            inverse = 1.0 / jnp.sum(den[m, rows(t)], axis=1, keepdims=True)
            alive = jnp.broadcast_to(exits[q_from[m], t : t + 1], (TILE, TILE)) > 0
            for lanes in (pl.ds(0, TILE), pl.ds(TILE, TILE)):
                o_send[m, rows(t), lanes] = jnp.where(
                    alive, acc[m, rows(t), lanes] * inverse, 0.0
                ).astype(jnp.bfloat16)
            if m == 0:
                pl.when(home)(o_here(t).start)
                pl.when(jnp.logical_not(home))(o_copy(m, t).start)
            else:
                o_copy(m, t).start()

    both_parts(2 * PAIRS - 1)
    work(2 * PAIRS - 1, 1)
    finish(3)
    finish(2)
    work(2 * PAIRS - 1, 0)
    finish(1)
    finish(0)

    count_second.wait_recv()
    live_ref[...] = column[0] + column[2]

    for holds, copy in q_sends + kv_sends:
        pl.when(holds)(copy.wait_send)
    for offset in near:
        exit_copy(offset).wait_send()
    exit_on.wait_send()
    count_first.wait_send()
    count_second.wait_send()
    for way in range(2):
        four_forward(way, 0).wait_send()
        pl.when(core == way)(four_forward(way, 1).wait_send)

    @pl.when(home)
    def _():
        own_q_send.wait_send()
        for copy in own_y_sends:
            copy.wait_send()
        for t in range(TILES):
            own_copy(t).wait_send()
            o_here(t).wait()

    @pl.when(jnp.logical_not(home))
    def _():
        for t in range(TILES):
            o_copy(0, t).wait_send()

    def sent(slot, carry):
        owned = (slot == OWN_SLOT[0]) | (slot == OWN_SLOT[1]) | (slot == OWN_SLOT[2])

        @pl.when(jnp.logical_not(owned) | home)
        def _():
            f_copy(slot).wait_send()

        f_copy(SLOTS + slot).wait_send()

        @pl.when(jnp.logical_not(owned))
        def _():
            y_first(slot, 0).wait_send()

        y_second(slot, 0).wait_send()
        return carry

    lax.fori_loop(0, SLOTS, sent, 0)
    for m in range(1, 4):
        for t in range(TILES):
            o_copy(m, t).wait_send()
    for n in range(4):
        local = home & (2 * own_column + core == n)
        for t in range(TILES):

            @pl.when(jnp.logical_not(local))
            def _():
                remote(
                    o_send.at[0, rows(t)],
                    out_hbm.at[rows(t), pl.ds(n * HD, HD)],
                    o_out.at[0, t], o_in.at[n, t], sibling,
                ).wait_recv()


def body(queries, keys, values, exit_layer, tile_order):
    hbm = pl.BlockSpec(memory_space=pltpu.HBM)
    smem = pl.BlockSpec(memory_space=pltpu.SMEM)
    vmem = pl.BlockSpec(memory_space=pltpu.VMEM)
    bf16, f32, i32 = jnp.bfloat16, jnp.float32, jnp.int32
    dma = pltpu.SemaphoreType.DMA
    attended, live = pl.pallas_call(
        kernel,
        out_shape=(
            jax.ShapeDtypeStruct((ROWS, 4 * HD), bf16),
            jax.ShapeDtypeStruct((8, 128), i32),
        ),
        in_specs=[hbm, hbm, hbm, smem, smem],
        out_specs=(hbm, vmem),
        scratch_shapes=[
            pltpu.VMEM((4, ROWS, HD), bf16),
            pltpu.VMEM((2, 2, TILES, TILE, HD), bf16),
            pltpu.VMEM((4, ROWS, HD), bf16),
            pltpu.VMEM((2, 2 * SLOTS, TILE, HD), bf16),
            pltpu.VMEM((4, ROWS, HD), f32),
            pltpu.VMEM((4, ROWS, TILE), f32),
            pltpu.VMEM((SLOTS, TILE, HD), bf16),
            pltpu.VMEM((2, 2, TILE, HD), bf16),
            pltpu.VMEM((4, ROWS, HD), bf16),
            pltpu.VMEM((Z, 8, 128), i32),
            pltpu.VMEM((3, 8, 128), i32),
            pltpu.SMEM((2 * SLOTS,), i32),
            pltpu.SMEM((4 * TILES,), i32),
            dma((2, 2, TILES)),
            dma((4,)),
            dma((TILES, 2)),
            dma((1,)),
            dma((TILES, 2)),
            dma((2, SLOTS)),
            dma((SLOTS,)),
            dma((2, 2, 2)),
            dma((2, 2)),
            dma((2, 2)),
            dma((2 * SLOTS,)),
            dma((2 * SLOTS,)),
            dma((SLOTS,)),
            dma((SLOTS,)),
            dma((SLOTS,)),
            dma((SLOTS,)),
            dma((7,)),
            dma((4,)),
            dma((4, TILES)),
            dma((4, TILES)),
            dma((TILES,)),
            dma((Z,)),
            dma((Z,)),
            dma((2,)),
            dma((2,)),
        ],
        compiler_params=pltpu.CompilerParams(collective_id=0, has_side_effects=True),
        cost_estimate=pl.CostEstimate(
            flops=9_663_676_416, bytes_accessed=3_145_728, transcendentals=18_874_368
        ),
        name="attend",
    )(queries[0], keys[0], values[0], exit_layer, tile_order)
    return attended[None], live[0, :1]


def solution(mesh):
    parts = ("batch", "seq")
    return jax.shard_map(
        body,
        mesh=mesh,
        in_specs=(
            P(None, parts, "head"),
            P(None, parts, "head"),
            P(None, parts, "head"),
            P(parts),
            P("batch"),
        ),
        out_specs=(P(None, parts, "head"), P("batch")),
        check_vma=False,
    )
```

```python
import math

import jax
import jax.numpy as jnp
from jax import lax
from jax.experimental import pallas as pl
from jax.experimental.pallas import tpu as pltpu
from jax.sharding import PartitionSpec as P

MESH = pl.DeviceIdType.MESH
HD = 256
TILE = 128
ROWS = 384
TILES = 3
Z = 8
PAIRS = 12
SLOTS = 2 * PAIRS
SCORE_TO_TANH = 0.0625 / 50.0
TANH_TO_EXP2 = 50.0 * math.log2(math.e)

OWN_SLOT = (0, 1, 23)
FOUR_SLOT = (20, 22, 21)
FIRST_PAIR = {1: 1, 2: 4, 3: 7}
HELD_LAG = 2
END_LAG = 4
FOUR_STEP = 9
SEND_FIRST = (1,2,3)
SEND_AT = {1:(4,), 2:(5,), 3:(6,), 4:(7,), 5:(10,11), 6:(8,), 7:(9,)}


def slot_of(away, t, side):
    return 2 * (FIRST_PAIR[away] + t) + side


def slot_sources():
    found = {}
    for t in range(TILES):
        found[OWN_SLOT[t]] = (0, t)
        found[FOUR_SLOT[t]] = (4, t)
        for away in (1, 2, 3):
            found[slot_of(away, t, 0)] = (Z - away, t)
            found[slot_of(away, t, 1)] = (away, t)
    return found


def rows(t):
    return pl.ds(t * TILE, TILE)


def kernel(
    q_hbm, k_hbm, v_hbm, exit_ref, order_ref,
    out, live_ref,
    q_mine, kv_mine, q, kv, acc, den, y_held, four_held, o_send, exits, column, k_order, q_order,
    mine_in, q_mine_in, own_in, own_q_in, own_y_out, z_out, z_in, four_out, four_in, four_on, f_out, f_in,
    y_out, y_in, y_on, y_end, q_out, q_in, o_out, o_in, e_out, e_in, c_out, c_in,
):
    batch = lax.axis_index("batch")
    seq = lax.axis_index("seq")
    core = lax.axis_index("head")
    y_lo = lax.rem(batch, 2)
    y_hi = seq // Z
    z = lax.rem(seq, Z)
    hosted = lax.rem(z, 4)
    home = core == hosted // 2
    sibling = {"head": 1 - core}
    other_batch = batch + 1 - 2 * y_lo
    y_to = (
        {"batch": other_batch, "seq": lax.rem(y_hi + y_lo, 2) * Z + z},
        {"batch": other_batch, "seq": lax.rem(y_hi + 1 - y_lo, 2) * Z + z},
    )

    def chip(offset):
        return y_hi * Z + lax.rem(z + offset, Z)

    def remote(src, dst, sent, arrived, device):
        return pltpu.make_async_remote_copy(
            src_ref=src, dst_ref=dst, send_sem=sent, recv_sem=arrived,
            device_id=device, device_id_type=MESH,
        )

    def columns(n):
        return pl.ds(pl.multiple_of(n * HD, HD), HD)

    q_from = (0, Z - 1, 1, Z - 2 - 4 * core)

    own_column = lax.rem(hosted, 2)
    own_loads = [
        pltpu.make_async_copy(
            src.at[rows(t), columns(own_column)], kv.at[part, OWN_SLOT[t]], own_in.at[t, part]
        )
        for t in range(TILES)
        for part, src in ((0, k_hbm), (1, v_hbm))
    ]
    own_q_load = pltpu.make_async_copy(
        q_hbm.at[:, columns(2 * own_column + core)], q.at[0], own_q_in.at[0]
    )

    loads = [
        pltpu.make_async_copy(
            src.at[rows(t), pl.ds(j * HD, HD)], kv_mine.at[part, j, t], mine_in.at[part, j, t]
        )
        for t in range(TILES)
        for j in range(2)
        for part, src in ((0, k_hbm), (1, v_hbm))
    ] + [
        pltpu.make_async_copy(q_hbm.at[:, pl.ds(n * HD, HD)], q_mine.at[n], q_mine_in.at[n])
        for n in range(4)
    ]
    for load in loads:
        load.start()

    @pl.when(home)
    def _():
        for load in own_loads:
            load.start()
        own_q_load.start()

    sublane = lax.broadcasted_iota(jnp.int32, (8, 128), 0)
    mine = jnp.zeros((8, 128), jnp.int32)
    for t in range(TILES):
        mine = jnp.where(sublane == t, exit_ref[t], mine)
    exits[0] = mine

    barrier = pltpu.get_barrier_semaphore()
    near = (1, 2, 3, 5, 6, 7)
    for offset in near:
        for c in range(2):
            pl.semaphore_signal(
                barrier, inc=1, device_id={"seq": chip(offset), "head": c}, device_id_type=MESH
            )
    for peer in y_to:
        for c in range(2):
            pl.semaphore_signal(
                barrier, inc=1, device_id={**peer, "head": c}, device_id_type=MESH
            )
    pl.semaphore_signal(barrier, inc=1, device_id=sibling, device_id_type=MESH)
    for load in loads:
        load.wait()
    pl.semaphore_wait(barrier, 2 * len(near) + 5)

    def q_copy(n, offset, c, index):
        head = lax.rem(z + offset, 4)
        return remote(
            q_mine.at[2 * lax.rem(head, 2) + c],
            q.at[index],
            q_out.at[n],
            q_in.at[index],
            {"seq": chip(offset), "head": c},
        )

    q_sends = []
    for n, (offset, c, index) in enumerate(
        ((2, 0, 3), (6, 1, 3), (1, 0, 1), (1, 1, 1), (7, 0, 2), (7, 1, 2))
    ):
        q_sends.append((lax.rem(z + offset, 4) // 2 == core, q_copy(n, offset, c, index)))
    own_q_send = remote(
        q_mine.at[2 * own_column + 1 - core], q.at[0], q_out.at[6], q_in.at[0], sibling
    )
    own_y_sends = [
        remote(
            kv_mine.at[part, own_column, t], y_held.at[OWN_SLOT[t]],
            own_y_out.at[t, part], y_in.at[OWN_SLOT[t]],
            {**y_to[OWN_SLOT[t] % 2], "head": part},
        )
        for t in range(TILES)
        for part in range(2)
    ]

    @pl.when(home)
    def _():
        for copy in own_y_sends:
            copy.start()

    for holds, copy in q_sends:

        @pl.when(holds)
        def _():
            copy.start()

    pl.when(home)(own_q_send.start)

    def z_copies(away):
        found = []
        for t in range(TILES):
            for side in range(2):
                offset = away if side == 0 else Z - away
                head = lax.rem(z + offset, 4)
                for part in range(2):
                    slot = slot_of(away, t, side)
                    found.append((
                        head // 2 == core,
                        remote(
                            kv_mine.at[part, lax.rem(head, 2), t],
                            kv.at[part, slot],
                            z_out.at[part, slot],
                            z_in.at[slot],
                            {"seq": chip(offset), "head": part},
                        ),
                    ))
        return found

    def four_copies():
        found = []
        for n in range(2):
            for way in range(2):
                offset = 2 if way == 0 else Z - 2
                for part in range(2):
                    if n == 1 and part != way:
                        continue
                    t = 1 if n == 1 else 2 * way
                    found.append((
                        home,
                        remote(
                            kv_mine.at[part, own_column, t],
                            four_held.at[way, n],
                            four_out.at[way, n, part],
                            four_in.at[way, n],
                            {"seq": chip(offset), "head": part},
                        ),
                    ))
        return found

    by_pair = {}
    for away in (1, 2, 3):
        copies = z_copies(away)
        for t in range(TILES):
            by_pair[FIRST_PAIR[away] + t] = copies[4 * t : 4 * t + 4]
    four = four_copies()
    by_pair[10], by_pair[11] = four[:4], four[4:]
    kv_sends = [copy for copies in by_pair.values() for copy in copies]

    def start_all(copies):
        for holds, copy in copies:
            pl.when(holds)(copy.start)

    def f_copy(slot):
        return remote(
            kv.at[core, slot], kv.at[core, slot], f_out.at[slot], f_in.at[slot], sibling
        )

    def f_arrived(slot):
        return remote(
            kv.at[1 - core, slot], kv.at[1 - core, slot], f_out.at[slot], f_in.at[slot], sibling
        )

    def own_copy(t):
        slot = OWN_SLOT[t]
        return remote(
            kv.at[1 - core, slot], kv.at[1 - core, slot],
            z_out.at[0, slot], z_in.at[slot], sibling,
        )

    def z_arrived(slot):
        return remote(
            kv.at[core, slot], kv.at[core, slot], f_out.at[slot], z_in.at[slot], sibling
        )

    def y_first(slot, side):
        return remote(
            kv.at[core, slot], y_held.at[slot], y_out.at[slot], y_in.at[slot], y_to[side]
        )

    def y_second(slot, side):
        return remote(
            y_held.at[slot], kv.at[core, SLOTS + slot], y_on.at[slot], y_end.at[slot], y_to[side]
        )

    def four_forward(way, n):
        slot = FOUR_SLOT[1] if n == 1 else FOUR_SLOT[2 * way]
        return remote(
            four_held.at[way, n], kv.at[core, slot], four_on.at[way, n], z_in.at[slot],
            {"seq": chip(2 if way == 0 else Z - 2)},
        )

    for pair in SEND_FIRST:
        start_all(by_pair[pair])

    def exit_copy(offset):
        back = Z - offset
        return remote(
            exits.at[0], exits.at[back], e_out.at[offset], e_in.at[back], {"seq": chip(offset)}
        )

    exit_on = remote(exits.at[2], exits.at[4], e_out.at[4], e_in.at[4], {"seq": chip(Z - 2)})
    for offset in near:
        exit_copy(offset).start()

    @pl.when(home)
    def _():
        for load in own_loads:
            load.wait()
        for t in range(TILES):
            own_copy(t).start()
            f_copy(OWN_SLOT[t]).start()

    @pl.when(jnp.logical_not(home))
    def _():
        for t in range(TILES):
            z_arrived(OWN_SLOT[t]).wait_recv()

    acc[...] = jnp.zeros_like(acc)
    den[...] = jnp.zeros_like(den)
    for slot, (offset, t) in slot_sources().items():
        there = lax.rem(z + offset, Z)
        for other in range(2):
            k_order[other * SLOTS + slot] = order_ref[
                (lax.rem(y_hi + other, 2) * Z + there) * TILES + t
            ]
    for m, offset in enumerate(q_from):
        for t in range(TILES):
            q_order[m * TILES + t] = order_ref[chip(offset) * TILES + t]

    ahead = lax.broadcasted_iota(jnp.int32, (TILE, TILE), 1) - lax.broadcasted_iota(
        jnp.int32, (TILE, TILE), 0
    )

    def work(pair, halves):
        key = kv[0, pl.ds(2 * pair, 2)].reshape(2 * TILE, HD)
        value = kv[1, pl.ds(2 * pair, 2)].reshape(2 * TILE, HD)
        left_order = k_order[2 * pair]
        right_order = k_order[2 * pair + 1]
        scores = [
            lax.dot_general(
                q[pl.ds(2 * half, 2)].reshape(2 * ROWS, HD), key, (((1,), (1,)), ((), ())),
                preferred_element_type=jnp.float32,
            )
            for half in halves
        ]
        for half, score in zip(halves, scores):
            blocks = []
            for m in range(2):
                for t in range(TILES):
                    lower = (m * TILES + t) * TILE
                    both = score[lower : lower + TILE]
                    both = jnp.exp2(jnp.tanh(both * SCORE_TO_TANH) * TANH_TO_EXP2)
                    mine = q_order[(2 * half + m) * TILES + t]
                    left = jnp.where(ahead <= (mine - left_order) * TILE, both[:, :TILE], 0.0)
                    right = jnp.where(ahead <= (mine - right_order) * TILE, both[:, TILE:], 0.0)
                    den[2 * half + m, rows(t)] += left + right
                    blocks.append(jnp.concatenate([left, right], axis=1).astype(jnp.bfloat16))
            product = jnp.dot(
                jnp.concatenate(blocks, axis=0), value, preferred_element_type=jnp.float32
            )
            acc[pl.ds(2 * half, 2)] += product.reshape(2, ROWS, HD)

    def both_parts(pair):
        for side in range(2):
            slot = 2 * pair + side
            owned = (slot == OWN_SLOT[0]) | (slot == OWN_SLOT[1]) | (slot == OWN_SLOT[2])

            @pl.when(jnp.logical_not(owned & home))
            def _():
                f_arrived(slot).wait_recv()

    def each_slot(p, act):
        for side in range(2):

            @pl.when(jnp.logical_not((p == PAIRS - 1) & (side == 1)))
            def _():
                act(2 * p + side, side)

        @pl.when(p == 0)
        def _():
            act(OWN_SLOT[2], 1)

    def arrive_z(slot, side):
        z_arrived(slot).wait_recv()
        f_copy(slot).start()
        y_first(slot, side).start()

    def arrive_held(slot, side):
        y_first(slot, side).wait_recv()
        y_second(slot, side).start()

    def arrive_y(slot, side):
        y_second(slot, side).wait_recv()
        f_copy(SLOTS + slot).start()

    def step(p, carry):
        @pl.when(p == FOUR_STEP)
        def _():
            for way in range(2):
                four_forward_in = remote(
                    four_held.at[way, 0], four_held.at[way, 0],
                    four_on.at[way, 0], four_in.at[way, 0], sibling,
                )
                four_forward_in.wait_recv()
                four_forward(way, 0).start()
            for way in range(2):

                @pl.when(core == way)
                def _():
                    remote(
                        four_held.at[way, 1], four_held.at[way, 1],
                        four_on.at[way, 1], four_in.at[way, 1], sibling,
                    ).wait_recv()
                    four_forward(way, 1).start()

        @pl.when(p >= END_LAG)
        def _():
            each_slot(p - END_LAG, arrive_y)

        @pl.when((p >= HELD_LAG) & (p < PAIRS + HELD_LAG))
        def _():
            each_slot(p - HELD_LAG, arrive_held)

        @pl.when((p >= 1) & (p <= PAIRS - 1))
        def _():
            each_slot(p, arrive_z)

        for at, pairs in SEND_AT.items():

            @pl.when(p == at)
            def _():
                for pair in pairs:
                    start_all(by_pair[pair])

        @pl.when(p == 1)
        def _():
            pl.when(home)(own_q_load.wait)
            for m in range(4):

                @pl.when(jnp.logical_not(home) if m == 0 else m > 0)
                def _():
                    remote(q.at[m], q.at[m], q_out.at[m], q_in.at[m], sibling).wait_recv()

        @pl.when((p >= 1) & (p <= PAIRS))
        def _():
            both_parts(p - 1)

        @pl.when(p > END_LAG)
        def _():
            both_parts(PAIRS + p - END_LAG - 1)

        first = jnp.where((p >= 1) & (p <= PAIRS), 0, 1)
        last = jnp.where(p > END_LAG, 2, 1)

        def item(n, c):
            work(jnp.where(n < 1, p - 1, PAIRS + p - END_LAG - 1), (0, 1))
            return c

        lax.fori_loop(first, last, item, 0)

        @pl.when(p == 3)
        def _():
            remote(exits.at[2], exits.at[2], e_out.at[2], e_in.at[2], sibling).wait_recv()
            exit_on.start()

        @pl.when(p == 6)
        def _():
            for offset in (1, 3, 4, 5, 6, 7):
                remote(
                    exits.at[offset], exits.at[offset],
                    e_out.at[offset], e_in.at[offset], sibling,
                ).wait_recv()
            alive = jnp.zeros((8, 128), jnp.int32)
            for offset in range(Z):
                alive = alive + (exits[offset] > 0).astype(jnp.int32)
            column[0] = jnp.broadcast_to(jnp.sum(alive, axis=0, keepdims=True), (8, 128))

        pl.when(p == 7)(count_first.start)

        @pl.when(p == 9)
        def _():
            count_first.wait_recv()
            count_second.start()

        return carry

    count_first = remote(column.at[0], column.at[1], c_out.at[0], c_in.at[0], y_to[0])
    count_second = remote(column.at[1], column.at[2], c_out.at[1], c_in.at[1], y_to[0])

    lax.fori_loop(0, PAIRS + END_LAG, step, 0)

    def o_copy(m, t):
        return remote(
            o_send.at[m, rows(t)],
            out.at[rows(t), columns(2 * own_column + core)],
            o_out.at[m, t],
            o_in.at[2 * own_column + core, t],
            {"seq": chip(q_from[m]), "head": hosted // 2},
        )

    def finish(m):
        for t in range(TILES):
            inverse = 1.0 / jnp.sum(den[m, rows(t)], axis=1, keepdims=True)
            alive = jnp.broadcast_to(exits[q_from[m], t : t + 1], (TILE, TILE)) > 0
            for lanes in (pl.ds(0, TILE), pl.ds(TILE, TILE)):
                o_send[m, rows(t), lanes] = jnp.where(
                    alive, acc[m, rows(t), lanes] * inverse, 0.0
                ).astype(jnp.bfloat16)
            if m == 0:
                pl.when(jnp.logical_not(home))(o_copy(m, t).start)

                @pl.when(home)
                def _():
                    out[rows(t), columns(2 * own_column + core)] = o_send[m, rows(t)]

            else:
                o_copy(m, t).start()

    both_parts(2 * PAIRS - 1)
    work(2 * PAIRS - 1, (1,))
    finish(3)
    finish(2)
    work(2 * PAIRS - 1, (0,))
    finish(1)
    finish(0)

    count_second.wait_recv()
    live_ref[0] = jnp.max(column[0] + column[2])

    for holds, copy in q_sends + kv_sends:
        pl.when(holds)(copy.wait_send)
    for offset in near:
        exit_copy(offset).wait_send()
    exit_on.wait_send()
    count_first.wait_send()
    count_second.wait_send()
    for way in range(2):
        four_forward(way, 0).wait_send()
        pl.when(core == way)(four_forward(way, 1).wait_send)

    @pl.when(home)
    def _():
        own_q_send.wait_send()
        for copy in own_y_sends:
            copy.wait_send()
        for t in range(TILES):
            own_copy(t).wait_send()

    @pl.when(jnp.logical_not(home))
    def _():
        for t in range(TILES):
            o_copy(0, t).wait_send()

    def sent(slot, carry):
        owned = (slot == OWN_SLOT[0]) | (slot == OWN_SLOT[1]) | (slot == OWN_SLOT[2])

        @pl.when(jnp.logical_not(owned) | home)
        def _():
            f_copy(slot).wait_send()

        f_copy(SLOTS + slot).wait_send()

        @pl.when(jnp.logical_not(owned))
        def _():
            y_first(slot, 0).wait_send()

        y_second(slot, 0).wait_send()
        return carry

    lax.fori_loop(0, SLOTS, sent, 0)
    for m in range(1, 4):
        for t in range(TILES):
            o_copy(m, t).wait_send()
    for n in range(4):
        local = home & (2 * own_column + core == n)
        for t in range(TILES):

            @pl.when(jnp.logical_not(local))
            def _():
                remote(
                    o_send.at[0, rows(t)],
                    out.at[rows(t), pl.ds(n * HD, HD)],
                    o_out.at[0, t], o_in.at[n, t], sibling,
                ).wait_recv()


def body(queries, keys, values, exit_layer, tile_order):
    hbm = pl.BlockSpec(memory_space=pltpu.HBM)
    smem = pl.BlockSpec(memory_space=pltpu.SMEM)
    bf16, f32, i32 = jnp.bfloat16, jnp.float32, jnp.int32
    dma = pltpu.SemaphoreType.DMA
    attended, live = pl.pallas_call(
        kernel,
        out_shape=(
            pltpu.VMEM((ROWS, 4 * HD), bf16),
            jax.ShapeDtypeStruct((1,), i32),
        ),
        in_specs=[hbm, hbm, hbm, smem, smem],
        out_specs=(pl.BlockSpec(memory_space=pltpu.VMEM), smem),
        scratch_shapes=[
            pltpu.VMEM((4, ROWS, HD), bf16),
            pltpu.VMEM((2, 2, TILES, TILE, HD), bf16),
            pltpu.VMEM((4, ROWS, HD), bf16),
            pltpu.VMEM((2, 2 * SLOTS, TILE, HD), bf16),
            pltpu.VMEM((4, ROWS, HD), f32),
            pltpu.VMEM((4, ROWS, TILE), f32),
            pltpu.VMEM((SLOTS, TILE, HD), bf16),
            pltpu.VMEM((2, 2, TILE, HD), bf16),
            pltpu.VMEM((4, ROWS, HD), bf16),
            pltpu.VMEM((Z, 8, 128), i32),
            pltpu.VMEM((3, 8, 128), i32),
            pltpu.SMEM((2 * SLOTS,), i32),
            pltpu.SMEM((4 * TILES,), i32),
            dma((2, 2, TILES)),
            dma((4,)),
            dma((TILES, 2)),
            dma((1,)),
            dma((TILES, 2)),
            dma((2, SLOTS)),
            dma((SLOTS,)),
            dma((2, 2, 2)),
            dma((2, 2)),
            dma((2, 2)),
            dma((2 * SLOTS,)),
            dma((2 * SLOTS,)),
            dma((SLOTS,)),
            dma((SLOTS,)),
            dma((SLOTS,)),
            dma((SLOTS,)),
            dma((7,)),
            dma((4,)),
            dma((4, TILES)),
            dma((4, TILES)),
            dma((Z,)),
            dma((Z,)),
            dma((2,)),
            dma((2,)),
        ],
        compiler_params=pltpu.CompilerParams(collective_id=0, has_side_effects=True),
        cost_estimate=pl.CostEstimate(
            flops=9_663_676_416, bytes_accessed=3_145_728, transcendentals=18_874_368
        ),
        name="attend",
    )(queries[0], keys[0], values[0], exit_layer, tile_order)
    return attended[None], live


def solution(mesh):
    parts = ("batch", "seq")
    return jax.shard_map(
        body,
        mesh=mesh,
        in_specs=(
            P(None, parts, "head"),
            P(None, parts, "head"),
            P(None, parts, "head"),
            P(parts),
            P("batch"),
        ),
        out_specs=(P(None, parts, "head"), P("batch")),
        check_vma=False,
    )
```

```python
import math

import jax
import jax.numpy as jnp
from jax import lax
from jax.experimental import pallas as pl
from jax.experimental.pallas import tpu as pltpu
from jax.sharding import PartitionSpec as P

MESH = pl.DeviceIdType.MESH
HD = 256
TILE = 128
ROWS = 384
TILES = 3
Z = 8
PAIRS = 12
SLOTS = 2 * PAIRS
SCORE_TO_TANH = 0.0625 / 50.0
TANH_TO_EXP2 = 50.0 * math.log2(math.e)

OWN_SLOT = (0, 1, 23)
FOUR_SLOT = (20, 22, 21)
FIRST_PAIR = {1: 1, 2: 4, 3: 7}
HELD_LAG = 2
END_LAG = 5
FOUR_STEP = 9
SEND_FIRST = (1,2,3)
SEND_AT = {1:(4,), 2:(5,), 3:(6,), 4:(7,), 5:(10,11), 6:(8,), 7:(9,)}


def slot_of(away, t, side):
    return 2 * (FIRST_PAIR[away] + t) + side


def slot_sources():
    found = {}
    for t in range(TILES):
        found[OWN_SLOT[t]] = (0, t)
        found[FOUR_SLOT[t]] = (4, t)
        for away in (1, 2, 3):
            found[slot_of(away, t, 0)] = (Z - away, t)
            found[slot_of(away, t, 1)] = (away, t)
    return found


def rows(t):
    return pl.ds(t * TILE, TILE)


def kernel(
    q_hbm, k_hbm, v_hbm, exit_ref, order_ref,
    out, live_ref,
    q_mine, kv_mine, q, kv, acc, den, y_held, four_held, o_send, exits, column, k_order, q_order,
    mine_in, q_mine_in, own_in, own_q_in, own_y_out, z_out, z_in, four_out, four_in, four_on, f_out, f_in,
    y_out, y_in, y_on, y_end, q_out, q_in, o_out, o_in, e_out, e_in, c_out, c_in,
):
    batch = lax.axis_index("batch")
    seq = lax.axis_index("seq")
    core = lax.axis_index("head")
    y_lo = lax.rem(batch, 2)
    y_hi = seq // Z
    z = lax.rem(seq, Z)
    hosted = lax.rem(z, 4)
    home = core == hosted // 2
    sibling = {"head": 1 - core}
    other_batch = batch + 1 - 2 * y_lo
    y_to = (
        {"batch": other_batch, "seq": lax.rem(y_hi + y_lo, 2) * Z + z},
        {"batch": other_batch, "seq": lax.rem(y_hi + 1 - y_lo, 2) * Z + z},
    )

    def chip(offset):
        return y_hi * Z + lax.rem(z + offset, Z)

    def remote(src, dst, sent, arrived, device):
        return pltpu.make_async_remote_copy(
            src_ref=src, dst_ref=dst, send_sem=sent, recv_sem=arrived,
            device_id=device, device_id_type=MESH,
        )

    def columns(n):
        return pl.ds(pl.multiple_of(n * HD, HD), HD)

    q_from = (0, Z - 1, 1, Z - 2 - 4 * core)

    own_column = lax.rem(hosted, 2)
    own_loads = [
        pltpu.make_async_copy(
            src.at[rows(t), columns(own_column)], kv.at[part, OWN_SLOT[t]], own_in.at[t, part]
        )
        for t in range(TILES)
        for part, src in ((0, k_hbm), (1, v_hbm))
    ]
    own_q_load = pltpu.make_async_copy(
        q_hbm.at[:, columns(2 * own_column + core)], q.at[0], own_q_in.at[0]
    )

    loads = [
        pltpu.make_async_copy(
            src.at[rows(t), pl.ds(j * HD, HD)], kv_mine.at[part, j, t], mine_in.at[part, j, t]
        )
        for t in range(TILES)
        for j in range(2)
        for part, src in ((0, k_hbm), (1, v_hbm))
    ] + [
        pltpu.make_async_copy(q_hbm.at[:, pl.ds(n * HD, HD)], q_mine.at[n], q_mine_in.at[n])
        for n in range(4)
    ]
    for load in loads:
        load.start()

    @pl.when(home)
    def _():
        for load in own_loads:
            load.start()
        own_q_load.start()

    sublane = lax.broadcasted_iota(jnp.int32, (8, 128), 0)
    mine = jnp.zeros((8, 128), jnp.int32)
    for t in range(TILES):
        mine = jnp.where(sublane == t, exit_ref[t], mine)
    exits[0] = mine

    barrier = pltpu.get_barrier_semaphore()
    near = (1, 2, 3, 5, 6, 7)
    for offset in near:
        for c in range(2):
            pl.semaphore_signal(
                barrier, inc=1, device_id={"seq": chip(offset), "head": c}, device_id_type=MESH
            )
    for peer in y_to:
        for c in range(2):
            pl.semaphore_signal(
                barrier, inc=1, device_id={**peer, "head": c}, device_id_type=MESH
            )
    pl.semaphore_signal(barrier, inc=1, device_id=sibling, device_id_type=MESH)
    for load in loads:
        load.wait()
    pl.semaphore_wait(barrier, 2 * len(near) + 5)

    def q_copy(n, offset, c, index):
        head = lax.rem(z + offset, 4)
        return remote(
            q_mine.at[2 * lax.rem(head, 2) + c],
            q.at[index],
            q_out.at[n],
            q_in.at[index],
            {"seq": chip(offset), "head": c},
        )

    q_sends = []
    for n, (offset, c, index) in enumerate(
        ((2, 0, 3), (6, 1, 3), (1, 0, 1), (1, 1, 1), (7, 0, 2), (7, 1, 2))
    ):
        q_sends.append((lax.rem(z + offset, 4) // 2 == core, q_copy(n, offset, c, index)))
    own_q_send = remote(
        q_mine.at[2 * own_column + 1 - core], q.at[0], q_out.at[6], q_in.at[0], sibling
    )
    own_y_sends = [
        remote(
            kv_mine.at[part, own_column, t], y_held.at[OWN_SLOT[t]],
            own_y_out.at[t, part], y_in.at[OWN_SLOT[t]],
            {**y_to[OWN_SLOT[t] % 2], "head": part},
        )
        for t in range(TILES)
        for part in range(2)
    ]

    @pl.when(home)
    def _():
        for copy in own_y_sends:
            copy.start()

    for holds, copy in q_sends:

        @pl.when(holds)
        def _():
            copy.start()

    pl.when(home)(own_q_send.start)

    def z_copies(away):
        found = []
        for t in range(TILES):
            for side in range(2):
                offset = away if side == 0 else Z - away
                head = lax.rem(z + offset, 4)
                for part in range(2):
                    slot = slot_of(away, t, side)
                    found.append((
                        head // 2 == core,
                        remote(
                            kv_mine.at[part, lax.rem(head, 2), t],
                            kv.at[part, slot],
                            z_out.at[part, slot],
                            z_in.at[slot],
                            {"seq": chip(offset), "head": part},
                        ),
                    ))
        return found

    def four_copies():
        found = []
        for n in range(2):
            for way in range(2):
                offset = 2 if way == 0 else Z - 2
                for part in range(2):
                    if n == 1 and part != way:
                        continue
                    t = 1 if n == 1 else 2 * way
                    found.append((
                        home,
                        remote(
                            kv_mine.at[part, own_column, t],
                            four_held.at[way, n],
                            four_out.at[way, n, part],
                            four_in.at[way, n],
                            {"seq": chip(offset), "head": part},
                        ),
                    ))
        return found

    by_pair = {}
    for away in (1, 2, 3):
        copies = z_copies(away)
        for t in range(TILES):
            by_pair[FIRST_PAIR[away] + t] = copies[4 * t : 4 * t + 4]
    four = four_copies()
    by_pair[10], by_pair[11] = four[:4], four[4:]
    kv_sends = [copy for copies in by_pair.values() for copy in copies]

    def start_all(copies):
        for holds, copy in copies:
            pl.when(holds)(copy.start)

    def f_copy(slot):
        return remote(
            kv.at[core, slot], kv.at[core, slot], f_out.at[slot], f_in.at[slot], sibling
        )

    def f_arrived(slot):
        return remote(
            kv.at[1 - core, slot], kv.at[1 - core, slot], f_out.at[slot], f_in.at[slot], sibling
        )

    def own_copy(t):
        slot = OWN_SLOT[t]
        return remote(
            kv.at[1 - core, slot], kv.at[1 - core, slot],
            z_out.at[0, slot], z_in.at[slot], sibling,
        )

    def z_arrived(slot):
        return remote(
            kv.at[core, slot], kv.at[core, slot], f_out.at[slot], z_in.at[slot], sibling
        )

    def y_first(slot, side):
        return remote(
            kv.at[core, slot], y_held.at[slot], y_out.at[slot], y_in.at[slot], y_to[side]
        )

    def y_second(slot, side):
        return remote(
            y_held.at[slot], kv.at[core, SLOTS + slot], y_on.at[slot], y_end.at[slot], y_to[side]
        )

    def four_forward(way, n):
        slot = FOUR_SLOT[1] if n == 1 else FOUR_SLOT[2 * way]
        return remote(
            four_held.at[way, n], kv.at[core, slot], four_on.at[way, n], z_in.at[slot],
            {"seq": chip(2 if way == 0 else Z - 2)},
        )

    for pair in SEND_FIRST:
        start_all(by_pair[pair])

    def exit_copy(offset):
        back = Z - offset
        return remote(
            exits.at[0], exits.at[back], e_out.at[offset], e_in.at[back], {"seq": chip(offset)}
        )

    exit_on = remote(exits.at[2], exits.at[4], e_out.at[4], e_in.at[4], {"seq": chip(Z - 2)})
    for offset in near:
        exit_copy(offset).start()

    @pl.when(home)
    def _():
        for load in own_loads:
            load.wait()
        for t in range(TILES):
            own_copy(t).start()
            f_copy(OWN_SLOT[t]).start()

    @pl.when(jnp.logical_not(home))
    def _():
        for t in range(TILES):
            z_arrived(OWN_SLOT[t]).wait_recv()

    acc[...] = jnp.zeros_like(acc)
    den[...] = jnp.zeros_like(den)
    for slot, (offset, t) in slot_sources().items():
        there = lax.rem(z + offset, Z)
        for other in range(2):
            k_order[other * SLOTS + slot] = order_ref[
                (lax.rem(y_hi + other, 2) * Z + there) * TILES + t
            ]
    for m, offset in enumerate(q_from):
        for t in range(TILES):
            q_order[m * TILES + t] = order_ref[chip(offset) * TILES + t]

    ahead = lax.broadcasted_iota(jnp.int32, (TILE, TILE), 1) - lax.broadcasted_iota(
        jnp.int32, (TILE, TILE), 0
    )

    def work(pair, halves):
        key = kv[0, pl.ds(2 * pair, 2)].reshape(2 * TILE, HD)
        value = kv[1, pl.ds(2 * pair, 2)].reshape(2 * TILE, HD)
        left_order = k_order[2 * pair]
        right_order = k_order[2 * pair + 1]
        scores = [
            lax.dot_general(
                q[pl.ds(2 * half, 2)].reshape(2 * ROWS, HD), key, (((1,), (1,)), ((), ())),
                preferred_element_type=jnp.float32,
            )
            for half in halves
        ]
        for half, score in zip(halves, scores):
            blocks = []
            for m in range(2):
                for t in range(TILES):
                    lower = (m * TILES + t) * TILE
                    both = score[lower : lower + TILE]
                    both = jnp.exp2(jnp.tanh(both * SCORE_TO_TANH) * TANH_TO_EXP2)
                    mine = q_order[(2 * half + m) * TILES + t]
                    left = jnp.where(ahead <= (mine - left_order) * TILE, both[:, :TILE], 0.0)
                    right = jnp.where(ahead <= (mine - right_order) * TILE, both[:, TILE:], 0.0)
                    den[2 * half + m, rows(t)] += left + right
                    blocks.append(jnp.concatenate([left, right], axis=1).astype(jnp.bfloat16))
            product = jnp.dot(
                jnp.concatenate(blocks, axis=0), value, preferred_element_type=jnp.float32
            )
            acc[pl.ds(2 * half, 2)] += product.reshape(2, ROWS, HD)

    def both_parts(pair):
        for side in range(2):
            slot = 2 * pair + side
            owned = (slot == OWN_SLOT[0]) | (slot == OWN_SLOT[1]) | (slot == OWN_SLOT[2])

            @pl.when(jnp.logical_not(owned & home))
            def _():
                f_arrived(slot).wait_recv()

    def each_slot(p, act):
        for side in range(2):

            @pl.when(jnp.logical_not((p == PAIRS - 1) & (side == 1)))
            def _():
                act(2 * p + side, side)

        @pl.when(p == 0)
        def _():
            act(OWN_SLOT[2], 1)

    def arrive_z(slot, side):
        z_arrived(slot).wait_recv()
        f_copy(slot).start()
        y_first(slot, side).start()

    def arrive_held(slot, side):
        y_first(slot, side).wait_recv()
        y_second(slot, side).start()

    def arrive_y(slot, side):
        y_second(slot, side).wait_recv()
        f_copy(SLOTS + slot).start()

    def step(p, carry):
        @pl.when(p == FOUR_STEP)
        def _():
            for way in range(2):
                four_forward_in = remote(
                    four_held.at[way, 0], four_held.at[way, 0],
                    four_on.at[way, 0], four_in.at[way, 0], sibling,
                )
                four_forward_in.wait_recv()
                four_forward(way, 0).start()
            for way in range(2):

                @pl.when(core == way)
                def _():
                    remote(
                        four_held.at[way, 1], four_held.at[way, 1],
                        four_on.at[way, 1], four_in.at[way, 1], sibling,
                    ).wait_recv()
                    four_forward(way, 1).start()

        @pl.when(p >= END_LAG)
        def _():
            each_slot(p - END_LAG, arrive_y)

        @pl.when(p > END_LAG)
        def _():
            both_parts(PAIRS + p - END_LAG - 1)
            work(PAIRS + p - END_LAG - 1, (0, 1))

        @pl.when((p >= HELD_LAG) & (p < PAIRS + HELD_LAG))
        def _():
            each_slot(p - HELD_LAG, arrive_held)

        @pl.when((p >= 1) & (p <= PAIRS - 1))
        def _():
            each_slot(p, arrive_z)

        for at, pairs in SEND_AT.items():

            @pl.when(p == at)
            def _():
                for pair in pairs:
                    start_all(by_pair[pair])

        @pl.when(p == 1)
        def _():
            pl.when(home)(own_q_load.wait)
            for m in range(4):

                @pl.when(jnp.logical_not(home) if m == 0 else m > 0)
                def _():
                    remote(q.at[m], q.at[m], q_out.at[m], q_in.at[m], sibling).wait_recv()

        @pl.when((p >= 1) & (p <= PAIRS))
        def _():
            both_parts(p - 1)
            work(p - 1, (0, 1))

        @pl.when(p == 3)
        def _():
            remote(exits.at[2], exits.at[2], e_out.at[2], e_in.at[2], sibling).wait_recv()
            exit_on.start()

        @pl.when(p == 6)
        def _():
            for offset in (1, 3, 4, 5, 6, 7):
                remote(
                    exits.at[offset], exits.at[offset],
                    e_out.at[offset], e_in.at[offset], sibling,
                ).wait_recv()
            alive = jnp.zeros((8, 128), jnp.int32)
            for offset in range(Z):
                alive = alive + (exits[offset] > 0).astype(jnp.int32)
            column[0] = jnp.broadcast_to(jnp.sum(alive, axis=0, keepdims=True), (8, 128))

        pl.when(p == 7)(count_first.start)

        @pl.when(p == 9)
        def _():
            count_first.wait_recv()
            count_second.start()

        return carry

    count_first = remote(column.at[0], column.at[1], c_out.at[0], c_in.at[0], y_to[0])
    count_second = remote(column.at[1], column.at[2], c_out.at[1], c_in.at[1], y_to[0])

    lax.fori_loop(0, PAIRS + END_LAG, step, 0)

    def o_copy(m, t):
        return remote(
            o_send.at[m, rows(t)],
            out.at[rows(t), columns(2 * own_column + core)],
            o_out.at[m, t],
            o_in.at[2 * own_column + core, t],
            {"seq": chip(q_from[m]), "head": hosted // 2},
        )

    def finish(m):
        for t in range(TILES):
            inverse = 1.0 / jnp.sum(den[m, rows(t)], axis=1, keepdims=True)
            alive = jnp.broadcast_to(exits[q_from[m], t : t + 1], (TILE, TILE)) > 0
            for lanes in (pl.ds(0, TILE), pl.ds(TILE, TILE)):
                o_send[m, rows(t), lanes] = jnp.where(
                    alive, acc[m, rows(t), lanes] * inverse, 0.0
                ).astype(jnp.bfloat16)
            if m == 0:
                pl.when(jnp.logical_not(home))(o_copy(m, t).start)

                @pl.when(home)
                def _():
                    out[rows(t), columns(2 * own_column + core)] = o_send[m, rows(t)]

            else:
                o_copy(m, t).start()

    both_parts(2 * PAIRS - 1)
    work(2 * PAIRS - 1, (1,))
    finish(3)
    finish(2)
    work(2 * PAIRS - 1, (0,))
    finish(1)
    finish(0)

    count_second.wait_recv()
    live_ref[0] = jnp.max(column[0] + column[2])

    for holds, copy in q_sends + kv_sends:
        pl.when(holds)(copy.wait_send)
    for offset in near:
        exit_copy(offset).wait_send()
    exit_on.wait_send()
    count_first.wait_send()
    count_second.wait_send()
    for way in range(2):
        four_forward(way, 0).wait_send()
        pl.when(core == way)(four_forward(way, 1).wait_send)

    @pl.when(home)
    def _():
        own_q_send.wait_send()
        for copy in own_y_sends:
            copy.wait_send()
        for t in range(TILES):
            own_copy(t).wait_send()

    @pl.when(jnp.logical_not(home))
    def _():
        for t in range(TILES):
            o_copy(0, t).wait_send()

    def sent(slot, carry):
        owned = (slot == OWN_SLOT[0]) | (slot == OWN_SLOT[1]) | (slot == OWN_SLOT[2])

        @pl.when(jnp.logical_not(owned) | home)
        def _():
            f_copy(slot).wait_send()

        f_copy(SLOTS + slot).wait_send()

        @pl.when(jnp.logical_not(owned))
        def _():
            y_first(slot, 0).wait_send()

        y_second(slot, 0).wait_send()
        return carry

    lax.fori_loop(0, SLOTS, sent, 0)
    for m in range(1, 4):
        for t in range(TILES):
            o_copy(m, t).wait_send()
    for n in range(4):
        local = home & (2 * own_column + core == n)
        for t in range(TILES):

            @pl.when(jnp.logical_not(local))
            def _():
                remote(
                    o_send.at[0, rows(t)],
                    out.at[rows(t), pl.ds(n * HD, HD)],
                    o_out.at[0, t], o_in.at[n, t], sibling,
                ).wait_recv()


def body(queries, keys, values, exit_layer, tile_order):
    hbm = pl.BlockSpec(memory_space=pltpu.HBM)
    smem = pl.BlockSpec(memory_space=pltpu.SMEM)
    bf16, f32, i32 = jnp.bfloat16, jnp.float32, jnp.int32
    dma = pltpu.SemaphoreType.DMA
    attended, live = pl.pallas_call(
        kernel,
        out_shape=(
            pltpu.VMEM((ROWS, 4 * HD), bf16),
            jax.ShapeDtypeStruct((1,), i32),
        ),
        in_specs=[hbm, hbm, hbm, smem, smem],
        out_specs=(pl.BlockSpec(memory_space=pltpu.VMEM), smem),
        scratch_shapes=[
            pltpu.VMEM((4, ROWS, HD), bf16),
            pltpu.VMEM((2, 2, TILES, TILE, HD), bf16),
            pltpu.VMEM((4, ROWS, HD), bf16),
            pltpu.VMEM((2, 2 * SLOTS, TILE, HD), bf16),
            pltpu.VMEM((4, ROWS, HD), f32),
            pltpu.VMEM((4, ROWS, TILE), f32),
            pltpu.VMEM((SLOTS, TILE, HD), bf16),
            pltpu.VMEM((2, 2, TILE, HD), bf16),
            pltpu.VMEM((4, ROWS, HD), bf16),
            pltpu.VMEM((Z, 8, 128), i32),
            pltpu.VMEM((3, 8, 128), i32),
            pltpu.SMEM((2 * SLOTS,), i32),
            pltpu.SMEM((4 * TILES,), i32),
            dma((2, 2, TILES)),
            dma((4,)),
            dma((TILES, 2)),
            dma((1,)),
            dma((TILES, 2)),
            dma((2, SLOTS)),
            dma((SLOTS,)),
            dma((2, 2, 2)),
            dma((2, 2)),
            dma((2, 2)),
            dma((2 * SLOTS,)),
            dma((2 * SLOTS,)),
            dma((SLOTS,)),
            dma((SLOTS,)),
            dma((SLOTS,)),
            dma((SLOTS,)),
            dma((7,)),
            dma((4,)),
            dma((4, TILES)),
            dma((4, TILES)),
            dma((Z,)),
            dma((Z,)),
            dma((2,)),
            dma((2,)),
        ],
        compiler_params=pltpu.CompilerParams(collective_id=0, has_side_effects=True),
        cost_estimate=pl.CostEstimate(
            flops=9_663_676_416, bytes_accessed=3_145_728, transcendentals=18_874_368
        ),
        name="attend",
    )(queries[0], keys[0], values[0], exit_layer, tile_order)
    return attended[None], live


def solution(mesh):
    parts = ("batch", "seq")
    return jax.shard_map(
        body,
        mesh=mesh,
        in_specs=(
            P(None, parts, "head"),
            P(None, parts, "head"),
            P(None, parts, "head"),
            P(parts),
            P("batch"),
        ),
        out_specs=(P(None, parts, "head"), P("batch")),
        check_vma=False,
    )
```
